32 devices in a mesh: prow: 4 (over y, core), pcol: 8 (over z, x).
Axes of the slice: x: 2, y: 2, z: 4, core: 2. Of those that a mesh axis runs over, the one named last changes fastest.
Arguments:
- tiles: bfloat16 [4, 8, 16, 256, 256], P('prow', 'pcol'), may hold values from -6 to 6
- tile_ids: int32 [4, 8, 16], P('prow', 'pcol'), may hold values from 0 to 127, as said below
- counts: int32 [4, 8], P('prow', 'pcol'), may hold values from 1 to 16, as said below
- pivots: int32 [256], replicated, may hold values from 0 to 16383, as said below
- l_inverse: bfloat16 [256, 256], P(None, 'pcol'), may hold values from -1 to 1, as said below
- u_inverse: bfloat16 [256, 256], P('prow'), may hold values from -0.125 to 0.5, as said below
Outputs:
- factored: bfloat16 [4, 8, 16, 256, 256], P('prow', 'pcol')
The draws below stay inside these ranges and needn't reach their ends.
Inputs may be any that keep to these rules, and one draw needn't show every extreme that they name: Live slot s of device (p, q) holds local tile row tile_ids[p, q, s] // 8 and local tile column tile_ids[p, q, s] % 8; live codes of one device are distinct, padded slots hold arbitrary codes. Let R be the tile rows I >= 1 with tile (I, 0) held and C the tile columns J >= 1 with tile (0, J) held. Tile (0, 0) is held; on each prow index R takes the last one to 3 local tile rows, on each pcol index C takes the last one to 3 local tile columns, and both most counts are reached on some index. Every tile whose row is 0 or in R and whose column is 0 or in C is held; no other held tile lies in tile row 0, a tile row of R, or tile column 0. `counts`: some device has 16 live slots. Row r of tile row 0 and row pivots[r] change places; pivots[r] is r or a row of a tile row of R, and the values that differ from their r are distinct. `l_inverse`: lower triangular with unit diagonal. `u_inverse`: upper triangular with a positive diagonal.
All inputs are finite; a program needn't handle non-finite values.
Results may differ from the reference program's by a relative error of at most 0.0056.
Values may be sent and summed in bfloat16 or wider, within the bound.
A program may use at most 64 MiB of HBM per device.

```python
import jax
import jax.numpy as jnp
from jax import lax

TILE_SIDE = 256
LOCAL_ROWS = 16
LOCAL_COLS = 8
TILE_GRID = 64
TILE_SLOTS = 16
LOWER_MOST = 3
UPPER_MOST = 3
N_PROW = 4
N_PCOL = 8


def layout(key):
    base = jax.random.fold_in(key, 17)
    keys = jax.random.split(base, 9)
    prow_count = TILE_GRID // LOCAL_ROWS
    pcol_count = TILE_GRID // LOCAL_COLS
    positions = LOCAL_ROWS * LOCAL_COLS
    lower_count = jax.random.randint(keys[0], (prow_count,), 1, LOWER_MOST + 1)
    lower_count = lower_count.at[jax.random.randint(keys[1], (), 0, prow_count)].set(LOWER_MOST)
    upper_count = jax.random.randint(keys[2], (pcol_count,), 1, UPPER_MOST + 1)
    upper_count = upper_count.at[jax.random.randint(keys[3], (), 0, pcol_count)].set(UPPER_MOST)
    row_local = jnp.arange(LOCAL_ROWS, dtype=jnp.int32)
    col_local = jnp.arange(LOCAL_COLS, dtype=jnp.int32)
    lower_rows = row_local[None, :] >= LOCAL_ROWS - lower_count[:, None]
    upper_cols = col_local[None, :] >= LOCAL_COLS - upper_count[:, None]
    prow_first = (jnp.arange(prow_count)[:, None] == 0) & (row_local[None, :] == 0)
    pcol_first = (jnp.arange(pcol_count)[:, None] == 0) & (col_local[None, :] == 0)
    row_set = lower_rows | prow_first
    col_set = upper_cols | pcol_first
    grid_shape = (prow_count, pcol_count, LOCAL_ROWS, LOCAL_COLS)
    structural = jnp.broadcast_to(row_set[:, None, :, None] & col_set[None, :, None, :], grid_shape)
    free = jnp.broadcast_to((~row_set)[:, None, :, None] & (~pcol_first)[None, :, None, :], grid_shape)
    structural = structural.reshape(prow_count, pcol_count, positions)
    free = free.reshape(prow_count, pcol_count, positions)
    base_count = jnp.sum(structural.astype(jnp.int32), axis=2)
    room = TILE_SLOTS - base_count
    extra = jax.random.randint(keys[4], (prow_count, pcol_count), 0, room + 1)
    full_row = jax.random.randint(keys[5], (), 0, prow_count)
    full_col = jax.random.randint(keys[6], (), 0, pcol_count)
    extra = extra.at[full_row, full_col].set(room[full_row, full_col])
    place = jnp.arange(positions, dtype=jnp.int32)
    noise = jax.random.randint(keys[7], (prow_count, pcol_count, positions), 0, 2 ** 20)
    score = jnp.where(free, noise * positions + place, -1 - place)
    rank = jnp.argsort(jnp.argsort(-score, axis=2), axis=2)
    chosen = free & (rank < extra[:, :, None])
    present = structural | chosen
    noise_two = jax.random.randint(keys[8], (prow_count, pcol_count, positions), 0, 2 ** 20)
    order_score = jnp.where(present, noise_two * positions + place, -1 - place)
    codes = jnp.argsort(-order_score, axis=2)[:, :, :TILE_SLOTS].astype(jnp.int32)
    live_count = (base_count + extra).astype(jnp.int32)
    return (codes, live_count, lower_rows)


def draw_tile_ids(key, part):
    return layout(key)[0]


def draw_counts(key, part):
    return layout(key)[1]


def draw_pivots(key, part):
    lower_rows = layout(key)[2]
    prow_count = TILE_GRID // LOCAL_ROWS
    total_rows = TILE_GRID * TILE_SIDE
    rows = jnp.arange(total_rows, dtype=jnp.int32)
    tile_row = rows // TILE_SIDE
    eligible = lower_rows[tile_row % prow_count, tile_row // prow_count]
    keys = jax.random.split(jax.random.fold_in(key, 29), 2)
    noise = jax.random.randint(keys[0], (total_rows,), 0, 2 ** 14)
    score = jnp.where(eligible, noise * total_rows + rows, -1)
    picked = jnp.argsort(-score)[:TILE_SIDE].astype(jnp.int32)
    stay = jax.random.randint(keys[1], (TILE_SIDE,), 0, 5) == 0
    return jnp.where(stay, jnp.arange(TILE_SIDE, dtype=jnp.int32), picked)


def draw_l_inverse(key, part):
    first = jax.random.fold_in(jax.random.fold_in(key, 41), 0)
    below = jnp.clip(jax.random.normal(first, (TILE_SIDE, TILE_SIDE), jnp.float32), -4.0, 4.0)
    below = below / jnp.sqrt(jnp.float32(TILE_SIDE))
    return (jnp.tril(below, -1) + jnp.eye(TILE_SIDE, dtype=jnp.float32)).astype(jnp.bfloat16)


def draw_u_inverse(key, part):
    first, second = jax.random.split(jax.random.fold_in(key, 53))
    above = jnp.clip(jax.random.normal(first, (TILE_SIDE, TILE_SIDE), jnp.float32), -4.0, 4.0)
    diagonal = jnp.exp(jax.random.uniform(second, (TILE_SIDE,), jnp.float32, jnp.log(0.5), jnp.log(2.0)))
    above = above / jnp.sqrt(jnp.float32(TILE_SIDE))
    upper = jnp.triu(above, 1) + jnp.diag(diagonal)
    return (upper / 8.0).astype(jnp.bfloat16)


def block_levels(rng, extent, cuts, least, top_value):
    level = 1.0
    for dim, blocks in cuts:
        draws = jax.random.uniform(jax.random.fold_in(jax.random.fold_in(rng, 6), dim), (blocks,), jnp.float32, least / len(cuts), top_value / len(cuts))
        level = level * jnp.repeat(jnp.exp(draws), extent[dim] // blocks).reshape((-1,) + (1,) * (len(extent) - 1 - dim))
    return level


def gaussian(key, dims, deviation, most, shards=(), kind=jnp.bfloat16):
    level = block_levels(key, dims, shards, -0.22, 0.18) if shards else 1.0
    array = jax.random.normal(key, dims, jnp.float32) * deviation * level
    return jnp.minimum(jnp.maximum(array, -most), most).astype(kind)


def setup_inputs(seed: int = 0) -> dict:
    key_of = jax.random.split(jax.random.key(seed), 7)
    tiles = gaussian(key_of[0], (N_PROW, N_PCOL, TILE_SLOTS, TILE_SIDE, TILE_SIDE), 1.0, 6.0, ((0, 4), (1, 8)))
    tile_ids = draw_tile_ids(jax.random.fold_in(key_of[6], 71), 0)
    counts = draw_counts(jax.random.fold_in(key_of[6], 71), 0)
    pivots = draw_pivots(jax.random.fold_in(key_of[6], 71), 0)
    l_inverse = draw_l_inverse(jax.random.fold_in(key_of[6], 71), 0)
    u_inverse = draw_u_inverse(jax.random.fold_in(key_of[6], 71), 0)
    return {"tiles": tiles, "tile_ids": tile_ids, "counts": counts, "pivots": pivots, "l_inverse": l_inverse, "u_inverse": u_inverse}


def reference(tiles, tile_ids, counts, pivots, l_inverse, u_inverse):
    side = TILE_SIDE
    total_rows = TILE_GRID * side
    device_total = N_PROW * N_PCOL * TILE_SLOTS
    flat = tiles.reshape(device_total, side, side)
    flat_rows = flat.reshape(device_total * side, side)
    shape = tile_ids.shape
    prow_of = jnp.broadcast_to(jnp.arange(N_PROW, dtype=jnp.int32)[:, None, None], shape).reshape(-1)
    pcol_of = jnp.broadcast_to(jnp.arange(N_PCOL, dtype=jnp.int32)[None, :, None], shape).reshape(-1)
    slot_of = jnp.broadcast_to(jnp.arange(TILE_SLOTS, dtype=jnp.int32)[None, None, :], shape).reshape(-1)
    alive = slot_of < jnp.broadcast_to(counts[:, :, None], shape).reshape(-1)
    codes = tile_ids.reshape(-1)
    glob_row = (prow_of + N_PROW * (codes // LOCAL_COLS)).astype(jnp.int32)
    glob_col = (pcol_of + N_PCOL * (codes % LOCAL_COLS)).astype(jnp.int32)
    table = jnp.full((TILE_GRID, TILE_GRID), -1, jnp.int32)
    table = table.at[jnp.where(alive, glob_row, TILE_GRID), glob_col].set(
        jnp.arange(device_total, dtype=jnp.int32), mode="drop")

    def fetch(slot, row):
        picked = flat_rows[jnp.maximum(slot, 0) * side + row]
        return jnp.where((slot >= 0)[..., None], picked, jnp.zeros_like(picked))

    every_col = jnp.arange(TILE_GRID, dtype=jnp.int32)
    row_range = jnp.arange(side, dtype=jnp.int32)
    new_slots = table[(pivots // side)[None, :], every_col[:, None]]
    new_top = fetch(new_slots, (pivots % side)[None, :])
    old_slots = jnp.broadcast_to(table[0, :][:, None], (TILE_GRID, side))
    old_top = fetch(old_slots, row_range[None, :])
    anchor_top = jnp.full((total_rows,), -1, jnp.int32).at[pivots].set(row_range)

    def primed_tile(tile, trow, tcol):
        anchor = lax.dynamic_slice_in_dim(anchor_top, (trow * side).astype(jnp.int32), side)
        moved = (anchor >= 0) & (trow >= 1)
        from_top = old_top[tcol][jnp.maximum(anchor, 0)]
        swapped = jnp.where(moved[:, None], from_top, tile)
        return jnp.where(trow == 0, new_top[tcol], swapped)

    lower_slot = table[:, 0]
    upper_slot = table[0, :]
    lower_present = (lower_slot >= 0) & (every_col >= 1)
    upper_present = (upper_slot >= 0) & (every_col >= 1)

    def lower_one(index):
        slot = lower_slot[index]
        tile = flat[jnp.maximum(slot, 0)]
        primed = primed_tile(tile, index, jnp.int32(0))
        value = jnp.dot(primed, u_inverse, preferred_element_type=jnp.float32).astype(jnp.bfloat16)
        return jnp.where(lower_present[index], value, jnp.zeros_like(value))

    def upper_one(index):
        value = jnp.dot(l_inverse, new_top[index], preferred_element_type=jnp.float32).astype(jnp.bfloat16)
        return jnp.where(upper_present[index], value, jnp.zeros_like(value))

    lower_panel = lax.map(lower_one, every_col)
    upper_row = lax.map(upper_one, every_col)

    def finish(index):
        tile = flat[index]
        trow = glob_row[index]
        tcol = glob_col[index]
        primed = primed_tile(tile, trow, tcol)

        def updated(unused):
            product = jnp.dot(lower_panel[trow], upper_row[tcol], preferred_element_type=jnp.float32)
            return (primed.astype(jnp.float32) - product).astype(jnp.bfloat16)

        def kept(unused):
            return primed

        interior = lax.cond(lower_present[trow] & upper_present[tcol], updated, kept, 0)
        value = jnp.where(trow == 0, jnp.where(tcol == 0, primed, upper_row[tcol]),
                          jnp.where(tcol == 0, lower_panel[trow], interior))
        return jnp.where(alive[index], value, jnp.zeros_like(value))

    result = lax.map(finish, jnp.arange(device_total, dtype=jnp.int32))
    return result.reshape(tiles.shape)
```

```python
import functools

import jax
import jax.numpy as jnp
from jax import lax
from jax.experimental import pallas as pl
from jax.experimental.pallas import tpu as pltpu
from jax.sharding import PartitionSpec as P

LOCAL_ROWS = 16
LOWER_MOST = 3
UPPER_MOST = 3
MESH = pl.DeviceIdType.MESH
NT = (((1,), (1,)), ((), ()))
TN = (((0,), (0,)), ((), ()))
FAR = 1 << 24


def dot(a, b, dims=None):
    if dims is None:
        return jnp.dot(a, b, preferred_element_type=jnp.float32)
    return lax.dot_general(a, b, dims, preferred_element_type=jnp.float32)


def kernel(
    rows, cols, grid_cols,
    ids_ref, counts_ref, piv_ref, l_ref, u_ref, tiles_ref,
    out_ref,
    store, part, old, send, recv, raw, top, lt, uf, new,
    tile_sem, ss, rs,
):
    side = piv_ref.shape[1]
    half = side // 2
    slots = tiles_ref.shape[2]
    zero_at = store.shape[0] - 1
    levels = rows.bit_length() - 1
    width = UPPER_MOST + 1
    height = LOWER_MOST + 1
    pieces = min(cols, 16)
    p = lax.axis_index("prow")
    q = lax.axis_index("pcol")
    core = lax.rem(p, 2)
    used = [0]
    ends = []

    def fresh(n=1):
        used[0] += n
        return used[0] - n

    def remote(src, dst, index, device):
        return pltpu.make_async_remote_copy(
            src_ref=src, dst_ref=dst, send_sem=ss.at[index], recv_sem=rs.at[index],
            device_id=device, device_id_type=MESH,
        )

    def guard(cond, fn):
        if cond is None:
            fn()
        else:
            pl.when(cond)(fn)

    def begin(cond, make):
        guard(cond, lambda: make().start())
        ends.append((cond, make))

    tile_copy = pltpu.make_async_copy(tiles_ref.at[0, 0], store.at[pl.ds(0, slots)], tile_sem)
    tile_copy.start()

    barrier = pltpu.get_barrier_semaphore()
    for d in range(1, rows):
        pl.semaphore_signal(barrier, inc=1, device_id={"prow": lax.rem(p + d, rows)}, device_id_type=MESH)
    for d in range(1, cols):
        pl.semaphore_signal(barrier, inc=1, device_id={"pcol": lax.rem(q + d, cols)}, device_id_type=MESH)

    first_row = LOCAL_ROWS - LOWER_MOST
    first_col = grid_cols - UPPER_MOST
    packed = [jnp.int32(0)] * height
    source = []
    live_count = counts_ref[0, 0]
    for s in range(slots):
        code = ids_ref[0, 0, s]
        row = code // grid_cols
        col = code - row * grid_cols
        live = s < live_count
        c = jnp.where((col == 0) & (q == 0), 0, jnp.where(col >= first_col, col - first_col + 1, -1))
        k = jnp.where((row == 0) & (p == 0), 0, jnp.where(row >= first_row, row - first_row + 1, -1))
        weight = jnp.int32(0)
        for j in range(width):
            weight = jnp.where(c == j, (s + 1) << (5 * j), weight)
        for i in range(height):
            packed[i] = packed[i] + jnp.where((k == i) & live, weight, 0)
        structural = (c >= 0) & (k >= 0)
        source.append(jnp.where(live, jnp.where(structural, slots + k * width + c, s), zero_at))

    def tile(k, c):
        slot = (packed[k] >> (5 * c)) & 31
        return store[jnp.where(slot > 0, slot - 1, zero_at)]

    store[zero_at] = jnp.zeros((side, side), jnp.bfloat16)
    piece = lt.shape[1]
    eye = (lax.broadcasted_iota(jnp.int32, (piece, piece), 0)
           == lax.broadcasted_iota(jnp.int32, (piece, piece), 1)).astype(jnp.float32).astype(jnp.bfloat16)
    lt[q] = dot(eye, l_ref[...], NT).astype(lt.dtype)
    u_rows = u_ref.shape[0]

    def u_part(at):
        return uf.at[pl.ds(pl.multiple_of(at * u_rows, 16), u_rows)]

    uf[pl.ds(pl.multiple_of(p * u_rows, 16), u_rows)] = u_ref[...]

    piv_lanes = jnp.broadcast_to(piv_ref[...], (side, side))
    piv_rows = piv_lanes.T
    lane = lax.broadcasted_iota(jnp.int32, (side, side), 1)
    sub = lax.broadcasted_iota(jnp.int32, (side, side), 0)
    base = [jnp.where(p == 0, 0, -FAR)]
    for i in range(LOWER_MOST):
        base.append((p + rows * (first_row + i)) * side)
    pick = [(piv_rows == lane + b).astype(jnp.float32).astype(jnp.bfloat16) for b in base]
    owner_high = lax.rem(piv_rows // side, rows) >= rows // 2

    pl.semaphore_wait(barrier, rows + cols - 2)

    l_sem = fresh(cols)
    u_sem = fresh(rows)
    for d in range(1, rows):
        begin(None, lambda d=d: remote(u_ref, u_part(p), u_sem + d, {"prow": lax.rem(p + d, rows)}))
    for d in range(1, cols):
        begin(None, lambda d=d: remote(lt.at[q], lt.at[q], l_sem + d, {"pcol": lax.rem(q + d, cols)}))
    tile_copy.wait()

    def row_cast(buf):
        length = buf.shape[0] // pieces
        scatter = fresh(pieces)
        gather = fresh(cols)

        def at(j):
            return buf.at[pl.ds(pl.multiple_of(j * length, 16), length)]

        def relay():
            for d in range(1, cols):
                to = lax.rem(q + d, cols)
                begin((to != 0) & (q < pieces),
                      lambda d=d, to=to: remote(at(q), at(q), gather + d, {"pcol": to}))

        def root():
            for j in range(1, pieces):
                begin(q == 0, lambda j=j: remote(at(j), at(j), scatter + j, {"pcol": j}))

        def arrive():
            for j in range(1, pieces):
                guard(q == j, lambda j=j: remote(at(j), at(j), scatter + j, {"pcol": 0}).wait_recv())

        def finish():
            for d in range(1, cols):
                frm = lax.rem(q + cols - d, cols)
                guard((q != 0) & (frm < pieces),
                      lambda d=d, frm=frm: remote(at(frm), at(frm), gather + d, {"pcol": frm}).wait_recv())

        return root, arrive, relay, finish

    raw_root, raw_arrive, raw_relay, raw_finish = row_cast(raw)
    top_root, top_arrive, top_relay, top_finish = row_cast(top)

    @pl.when(q == 0)
    def _():
        for i in range(LOWER_MOST):
            raw[pl.ds(i * side, side)] = tile(i + 1, 0)

    raw_root()

    def only(c):
        return (q == 0) if c == 0 else None

    def both(a, b):
        return b if a is None else (a if b is None else a & b)

    def part_rows(buf, at):
        return buf.at[pl.ds(pl.multiple_of(at * half, 16), half)]

    partner = {"prow": p + 1 - 2 * core}
    level0 = [fresh(2) for c in range(width)]
    for c in range(width):
        def contribute(c=c):
            total = dot(pick[0], tile(0, c))
            for k in range(1, height):
                total = total + dot(pick[k], tile(k, c))
            part[c] = total.astype(jnp.bfloat16)

            @pl.when(p == 0)
            def _():
                old[c] = tile(0, c)

        guard(only(c), contribute)
        begin(only(c), lambda c=c: remote(part.at[c], recv.at[0, c], level0[c], partner))
        begin(both(only(c), p == 0), lambda c=c: remote(old.at[c], old.at[c], level0[c] + 1, {"prow": 1}))

    def low(level):
        return p < (1 << level)

    def high(level):
        return (p >= (1 << level)) & (p < (2 << level))

    sems = {}

    def level_send(level, c):
        peer = {"prow": p + (1 << level) - 2 * (1 << level) * lax.rem(p // (1 << level), 2)}
        last = level == levels - 1
        sems[level, c] = fresh(4)
        index = sems[level, c]

        def build():
            if level == 1:
                @pl.when(p == 1)
                def _():
                    remote(old.at[c], old.at[c], level0[c] + 1, {"prow": 0}).wait_recv()
                remote(part.at[c], recv.at[0, c], level0[c], partner).wait_recv()
            total = part[c].astype(jnp.float32) + recv[level - 1, c].astype(jnp.float32)
            part_next = total.astype(jnp.bfloat16)
            send[level - 1, c] = part_next
            if last:
                @pl.when(p < rows // 2)
                def _():
                    new[c] = jnp.where(owner_high, old[c].astype(jnp.float32), total).astype(jnp.bfloat16)

                @pl.when(p >= rows // 2)
                def _():
                    new[c] = part_next

        guard(only(c), build)
        src = new.at[c] if last else send.at[level - 1, c]
        begin(only(c), lambda: remote(part_rows(src, core), part_rows(recv.at[level, c], core), index, peer))
        if not last:
            begin(both(only(c), low(level)),
                  lambda: remote(part_rows(old.at[c], core), part_rows(old.at[c], core), index + 1, peer))

    def level_forward(level, c):
        last = level == levels - 1
        index = sems[level, c]
        here = part_rows(recv.at[level, c], core)
        guard(only(c), lambda: remote(here, here, index, partner).wait_recv())
        begin(only(c), lambda: remote(here, here, index + 2, partner))
        if not last:
            mine = part_rows(old.at[c], core)
            guard(both(only(c), high(level)), lambda: remote(mine, mine, index + 1, partner).wait_recv())
            begin(both(only(c), high(level)), lambda: remote(mine, mine, index + 3, partner))

    def level_done(level, c):
        index = sems[level, c]
        there = part_rows(recv.at[level, c], 1 - core)
        guard(only(c), lambda: remote(there, there, index + 2, partner).wait_recv())
        if level < levels - 1:
            theirs = part_rows(old.at[c], 1 - core)
            guard(both(only(c), high(level)), lambda: remote(theirs, theirs, index + 3, partner).wait_recv())

    for level in range(1, levels):
        for c in range(width):
            if level > 1:
                def carry(c=c, level=level):
                    part[c] = send[level - 2, c]
                guard(only(c), carry)
            level_send(level, c)
        for c in range(width):
            level_forward(level, c)
        for c in range(width):
            level_done(level, c)
            if level == levels - 1 and c == 0:
                @pl.when((q == 0) & (p < rows // 2))
                def _():
                    top[...] = old[0]

                @pl.when((q == 0) & (p >= rows // 2))
                def _():
                    top[...] = recv[levels - 1, 0]

                top_root()
                guard(None, raw_arrive)
                raw_relay()
                top_arrive()
                top_relay()

    mine_high = p >= rows // 2
    for d in range(1, cols):
        frm = lax.rem(q + cols - d, cols)
        remote(lt.at[frm], lt.at[frm], l_sem + d, {"pcol": frm}).wait_recv()
    lower_t = lt[...].reshape(side, side).astype(jnp.bfloat16)

    same = (owner_high.astype(jnp.int32) == mine_high.astype(jnp.int32))

    def fresh_top(c):
        return jnp.where(same, send[levels - 2, c].astype(jnp.float32),
                         recv[levels - 1, c].astype(jnp.float32)).astype(jnp.bfloat16)

    @pl.when((q == 0) & (p == 0))
    def _():
        store[slots] = fresh_top(0)

    for c in range(1, width):
        store[slots + c] = dot(lower_t, fresh_top(c), TN).astype(jnp.bfloat16)

        @pl.when(mine_high)
        def _():
            old[c] = recv[levels - 1, c]

    def swap(k, block, source_rows):
        hit = piv_lanes == sub + base[k]
        moved = jnp.max(hit.astype(jnp.float32), axis=1, keepdims=True) > 0.5
        chosen = dot(hit.astype(jnp.float32).astype(jnp.bfloat16), source_rows)
        return jnp.where(moved, chosen, block.astype(jnp.float32))

    for d in range(1, rows):
        frm = lax.rem(p + rows - d, rows)
        remote(u_ref, u_part(frm), u_sem + d, {"prow": frm}).wait_recv()
    raw_finish()
    top_finish()
    for k in range(1, height):
        block = swap(k, raw[pl.ds((k - 1) * side, side)], top[...]).astype(jnp.bfloat16)
        lower = dot(block, uf[...]).astype(jnp.bfloat16)
        store[slots + k * width] = lower
        for c in range(1, width):
            value = swap(k, tile(k, c), old[c])
            store[slots + k * width + c] = (value - dot(lower, store[slots + c])).astype(jnp.bfloat16)

    for s in range(slots):
        out_ref[0, 0, s] = store[source[s]]
    for cond, make in ends:
        guard(cond, lambda make=make: make().wait_send())


def body(tiles, tile_ids, counts, pivots, l_inverse, u_inverse):
    rows = lax.axis_size("prow")
    cols = lax.axis_size("pcol")
    side = pivots.shape[0]
    slots = tiles.shape[2]
    grid_cols = LOCAL_ROWS * rows // cols
    levels = rows.bit_length() - 1
    width = UPPER_MOST + 1
    height = LOWER_MOST + 1
    piece = side // cols
    block = (side, side)
    pieces = min(cols, 16)
    count = rows + cols + 2 * (pieces + cols) + width * (2 + 4 * (levels - 1))
    kind = jnp.bfloat16
    vmem = pl.BlockSpec(memory_space=pltpu.VMEM)
    smem = pl.BlockSpec(memory_space=pltpu.SMEM)
    return pl.pallas_call(
        functools.partial(kernel, rows, cols, grid_cols),
        out_shape=jax.ShapeDtypeStruct(tiles.shape, tiles.dtype),
        in_specs=[smem, smem, vmem, vmem, vmem, pl.BlockSpec(memory_space=pl.ANY)],
        out_specs=vmem,
        scratch_shapes=[
            pltpu.VMEM((slots + height * width + 1,) + block, kind),
            pltpu.VMEM((width,) + block, kind),
            pltpu.VMEM((width,) + block, kind),
            pltpu.VMEM((levels - 1, width) + block, kind),
            pltpu.VMEM((levels, width) + block, kind),
            pltpu.VMEM((LOWER_MOST * side, side), kind),
            pltpu.VMEM(block, kind),
            pltpu.VMEM((cols, piece, side), kind if piece % 16 == 0 else jnp.float32),
            pltpu.VMEM(block, kind),
            pltpu.VMEM((width,) + block, kind),
            pltpu.SemaphoreType.DMA,
            pltpu.SemaphoreType.DMA((count,)),
            pltpu.SemaphoreType.DMA((count,)),
        ],
        compiler_params=pltpu.CompilerParams(
            collective_id=0, has_side_effects=True, vmem_limit_bytes=48 * 1024 * 1024
        ),
    )(tile_ids, counts, pivots.reshape(1, side), l_inverse, u_inverse, tiles)


def solution(mesh):
    placed = (
        P("prow", "pcol", None, None, None),
        P("prow", "pcol", None),
        P("prow", "pcol"),
        P(),
        P(None, "pcol"),
        P("prow", None),
    )
    return jax.shard_map(
        body,
        mesh=mesh,
        in_specs=placed,
        out_specs=P("prow", "pcol", None, None, None),
        check_vma=False,
    )
```

```python
import functools

import jax
import jax.numpy as jnp
from jax import lax
from jax.experimental import pallas as pl
from jax.experimental.pallas import tpu as pltpu
from jax.sharding import PartitionSpec as P

LOCAL_ROWS = 16
LOWER_MOST = 3
UPPER_MOST = 3
MESH = pl.DeviceIdType.MESH
NT = (((1,), (1,)), ((), ()))
TN = (((0,), (0,)), ((), ()))
FAR = 1 << 24


def dot(a, b, dims=None):
    if dims is None:
        return jnp.dot(a, b, preferred_element_type=jnp.float32)
    return lax.dot_general(a, b, dims, preferred_element_type=jnp.float32)


def kernel(
    rows, cols, grid_cols,
    ids_hbm, counts_hbm, piv_hbm, l_hbm, u_hbm, tiles_hbm,
    out_ref,
    ids_ref, counts_ref, piv_ref,
    store, part, old, send, recv, new, raw, top, lt, uf, corner,
    in_sem, ss, rs,
):
    side = piv_ref.shape[1]
    half = side // 2
    slots = tiles_hbm.shape[2]
    zero_at = store.shape[0] - 1
    levels = rows.bit_length() - 1
    width = UPPER_MOST + 1
    height = LOWER_MOST + 1
    pieces = min(cols, 16)
    panel_cols = range(1, width)
    p = lax.axis_index("prow")
    q = lax.axis_index("pcol")
    core = lax.rem(p, 2)
    used = [0]
    ends = []

    def fresh(n=1):
        used[0] += n
        return used[0] - n

    def remote(src, dst, index, device):
        return pltpu.make_async_remote_copy(
            src_ref=src, dst_ref=dst, send_sem=ss.at[index], recv_sem=rs.at[index],
            device_id=device, device_id_type=MESH,
        )

    def guard(cond, fn):
        if cond is None:
            fn()
        else:
            pl.when(cond)(fn)

    def begin(cond, make):
        guard(cond, lambda: make().start())
        ends.append((cond, make))

    def arrived(cond, make):
        guard(cond, lambda: make().wait_recv())

    def span(buf, at, length):
        return buf.at[pl.ds(pl.multiple_of(at * length, 16), length)]

    u_rows = u_hbm.shape[0]
    tile_copy = pltpu.make_async_copy(tiles_hbm.at[0, 0], store.at[pl.ds(0, slots)], in_sem.at[0])
    inputs = [
        pltpu.make_async_copy(ids_hbm, ids_ref, in_sem.at[1]),
        pltpu.make_async_copy(counts_hbm, counts_ref, in_sem.at[2]),
        pltpu.make_async_copy(piv_hbm, piv_ref, in_sem.at[3]),
        pltpu.make_async_copy(l_hbm, lt.at[q], in_sem.at[4]),
        pltpu.make_async_copy(u_hbm, span(uf, p, u_rows), in_sem.at[5]),
    ]
    for copy in inputs[:3]:
        copy.start()
    tile_copy.start()
    for copy in inputs[3:]:
        copy.start()

    barrier = pltpu.get_barrier_semaphore()
    for d in range(1, rows):
        pl.semaphore_signal(barrier, inc=1, device_id={"prow": lax.rem(p + d, rows)}, device_id_type=MESH)
    for d in range(1, cols):
        pl.semaphore_signal(barrier, inc=1, device_id={"pcol": lax.rem(q + d, cols)}, device_id_type=MESH)
    store[zero_at] = jnp.zeros((side, side), jnp.bfloat16)
    for copy in inputs:
        copy.wait()

    first_row = LOCAL_ROWS - LOWER_MOST
    first_col = grid_cols - UPPER_MOST
    packed = [jnp.int32(0)] * height
    source = []
    live_count = counts_ref[0, 0]
    for s in range(slots):
        code = ids_ref[0, 0, s]
        row = code // grid_cols
        col = code - row * grid_cols
        live = s < live_count
        c = jnp.where((col == 0) & (q == 0), 0, jnp.where(col >= first_col, col - first_col + 1, -1))
        k = jnp.where((row == 0) & (p == 0), 0, jnp.where(row >= first_row, row - first_row + 1, -1))
        weight = jnp.int32(0)
        for j in range(width):
            weight = jnp.where(c == j, (s + 1) << (5 * j), weight)
        for i in range(height):
            packed[i] = packed[i] + jnp.where((k == i) & live, weight, 0)
        structural = (c >= 0) & (k >= 0)
        source.append(jnp.where(live, jnp.where(structural, slots + k * width + c, s), zero_at))

    def tile(k, c):
        slot = (packed[k] >> (5 * c)) & 31
        return store[jnp.where(slot > 0, slot - 1, zero_at)]

    piv_lanes = jnp.broadcast_to(piv_ref[...], (side, side))
    piv_rows = piv_lanes.T
    lane = lax.broadcasted_iota(jnp.int32, (side, side), 1)
    sub = lax.broadcasted_iota(jnp.int32, (side, side), 0)
    base = [jnp.where(p == 0, 0, -FAR)]
    for i in range(LOWER_MOST):
        base.append((p + rows * (first_row + i)) * side)
    pick = [(piv_rows == lane + b).astype(jnp.float32).astype(jnp.bfloat16) for b in base]
    owner_high = lax.rem(piv_rows // side, rows) >= rows // 2
    mine_high = p >= rows // 2
    same = owner_high.astype(jnp.int32) == mine_high.astype(jnp.int32)

    tile_copy.wait()

    @pl.when(q == 0)
    def _():
        for i in range(LOWER_MOST):
            raw[pl.ds(i * side, side)] = tile(i + 1, 0)

        @pl.when(p == 0)
        def _():
            top[...] = tile(0, 0)

    pl.semaphore_wait(barrier, rows + cols - 2)

    top_piece = side // pieces
    raw_piece = LOWER_MOST * side // pieces
    top_scatter, raw_scatter = fresh(pieces), fresh(pieces)
    top_spread = fresh(rows)
    top_gather, raw_gather = fresh(cols), fresh(cols)
    for j in range(pieces - 1, 0, -1):
        begin((q == 0) & (p == 0), lambda j=j: remote(
            span(top, j, top_piece), span(top, j, top_piece), top_scatter + j, {"pcol": j}))
    for j in range(pieces - 1, 0, -1):
        begin(q == 0, lambda j=j: remote(
            span(raw, j, raw_piece), span(raw, j, raw_piece), raw_scatter + j, {"pcol": j}))

    partner = {"prow": p + 1 - 2 * core}
    level0 = [fresh(2) for c in range(width)]

    def contribute(c):
        total = dot(pick[0], tile(0, c))
        for k in range(1, height):
            total = total + dot(pick[k], tile(k, c))
        part[c] = total.astype(jnp.bfloat16)

    for c in panel_cols:
        contribute(c)

        @pl.when(p == 0)
        def _():
            old[c] = tile(0, c)

        begin(None, lambda c=c: remote(part.at[c], recv.at[0, c], level0[c], partner))
        begin(p == 0, lambda c=c: remote(old.at[c], old.at[c], level0[c] + 1, {"prow": 1}))

    def low(level):
        return p < (1 << level)

    def high(level):
        return (p >= (1 << level)) & (p < (2 << level))

    sems = {}

    def level_send(level, c):
        peer = {"prow": p + (1 << level) - 2 * (1 << level) * lax.rem(p // (1 << level), 2)}
        last = level == levels - 1
        sems[level, c] = fresh(4)
        index = sems[level, c]
        before = part if level == 1 else send.at[level - 2]
        if level == 1:
            arrived(p == 1, lambda: remote(old.at[c], old.at[c], level0[c] + 1, {"prow": 0}))
            arrived(None, lambda: remote(part.at[c], recv.at[0, c], level0[c], partner))
        total = before[c].astype(jnp.float32) + recv[level - 1, c].astype(jnp.float32)
        send[level - 1, c] = total.astype(jnp.bfloat16)
        if last:
            @pl.when(p < rows // 2)
            def _():
                new[c] = jnp.where(owner_high, old[c].astype(jnp.float32), total).astype(jnp.bfloat16)

            @pl.when(p >= rows // 2)
            def _():
                new[c] = total.astype(jnp.bfloat16)

        src = new.at[c] if last else send.at[level - 1, c]
        begin(None, lambda: remote(span(src, core, half), span(recv.at[level, c], core, half), index, peer))
        if not last:
            begin(low(level),
                  lambda: remote(span(old.at[c], core, half), span(old.at[c], core, half), index + 1, peer))

    def level_forward(level, c):
        index = sems[level, c]
        here = span(recv.at[level, c], core, half)
        arrived(None, lambda: remote(here, here, index, partner))
        begin(None, lambda: remote(here, here, index + 2, partner))
        if level < levels - 1:
            mine = span(old.at[c], core, half)
            arrived(high(level), lambda: remote(mine, mine, index + 1, partner))
            begin(high(level), lambda: remote(mine, mine, index + 3, partner))

    def level_done(level, c):
        index = sems[level, c]
        there = span(recv.at[level, c], 1 - core, half)
        arrived(None, lambda: remote(there, there, index + 2, partner))
        if level < levels - 1:
            theirs = span(old.at[c], 1 - core, half)
            arrived(high(level), lambda: remote(theirs, theirs, index + 3, partner))

    for c in panel_cols:
        level_send(1, c)

    for j in range(1, pieces):
        arrived((q == j) & (p == 0), lambda j=j: remote(
            span(top, j, top_piece), span(top, j, top_piece), top_scatter + j, {"pcol": 0}))
    mine_top = span(top, q, top_piece)
    for d in range(1, rows):
        begin((p == 0) & (q < pieces), lambda d=d: remote(mine_top, mine_top, top_spread + d, {"prow": d}))

    def top_relay(cond):
        for d in range(1, cols):
            to = lax.rem(q + d, cols)
            begin(cond & (q < pieces) & ((to != 0) | (p != 0)),
                  lambda d=d, to=to: remote(mine_top, mine_top, top_gather + d, {"pcol": to}))

    for j in range(1, pieces):
        arrived(q == j, lambda j=j: remote(
            span(raw, j, raw_piece), span(raw, j, raw_piece), raw_scatter + j, {"pcol": 0}))
    mine_raw = span(raw, q, raw_piece)
    for d in range(1, cols):
        to = lax.rem(q + d, cols)
        begin((q < pieces) & (to != 0),
              lambda d=d, to=to: remote(mine_raw, mine_raw, raw_gather + d, {"pcol": to}))
    for d in range(1, rows):
        arrived((p == d) & (q < pieces), lambda d=d: remote(mine_top, mine_top, top_spread + d, {"prow": 0}))
    top_relay(p >= 0)

    l_sem, u_sem, corner_sem = fresh(cols), fresh(rows), fresh(rows)
    for d in range(1, cols):
        begin(None, lambda d=d: remote(lt.at[q], lt.at[q], l_sem + d, {"pcol": lax.rem(q + d, cols)}))
    mine_u = span(uf, p, u_rows)
    for d in range(1, rows):
        begin(None, lambda d=d: remote(mine_u, mine_u, u_sem + d, {"prow": lax.rem(p + d, rows)}))

    @pl.when(q == 0)
    def _():
        contribute(0)

    for d in range(1, rows):
        begin((q == 0) & (p == d), lambda d=d: remote(part.at[0], corner.at[d - 1], corner_sem + d, {"prow": 0}))

    for level in range(1, levels):
        if level > 1:
            for c in panel_cols:
                level_send(level, c)
        for c in panel_cols:
            level_forward(level, c)
        if level < levels - 1:
            for c in panel_cols:
                level_done(level, c)

    for d in range(1, cols):
        frm = lax.rem(q + cols - d, cols)
        remote(lt.at[frm], lt.at[frm], l_sem + d, {"pcol": frm}).wait_recv()
    lower_t = lt[...].astype(jnp.float32).reshape(side, side).astype(jnp.bfloat16)

    hit = [piv_lanes == sub + b for b in base]
    moved = [jnp.max(h.astype(jnp.float32), axis=1, keepdims=True) > 0.5 for h in hit]
    choose = [h.astype(jnp.float32).astype(jnp.bfloat16) for h in hit]

    def swap(k, block, source_rows):
        return jnp.where(moved[k], dot(choose[k], source_rows), block.astype(jnp.float32)).astype(jnp.bfloat16)

    for c in panel_cols:
        level_done(levels - 1, c)
        fresh_top = jnp.where(same, send[levels - 2, c].astype(jnp.float32),
                              recv[levels - 1, c].astype(jnp.float32)).astype(jnp.bfloat16)
        store[slots + c] = dot(lower_t, fresh_top, TN).astype(jnp.bfloat16)

        @pl.when(mine_high)
        def _():
            old[c] = recv[levels - 1, c]

        for k in range(1, height):
            store[slots + k * width + c] = swap(k, tile(k, c), old[c])

    for d in range(1, rows):
        frm = lax.rem(p + rows - d, rows)
        there = span(uf, frm, u_rows)
        remote(there, there, u_sem + d, {"prow": frm}).wait_recv()

    @pl.when((q == 0) & (p == 0))
    def _():
        total = part[0].astype(jnp.float32)
        for d in range(1, rows):
            remote(part.at[0], corner.at[d - 1], corner_sem + d, {"prow": d}).wait_recv()
            total = total + corner[d - 1].astype(jnp.float32)
        store[slots] = total.astype(jnp.bfloat16)

    for d in range(1, cols):
        frm = lax.rem(q + cols - d, cols)
        arrived((frm < pieces) & ((q != 0) | (p != 0)), lambda d=d, frm=frm: remote(
            span(top, frm, top_piece), span(top, frm, top_piece), top_gather + d, {"pcol": frm}))
    for d in range(1, cols):
        frm = lax.rem(q + cols - d, cols)
        arrived((q != 0) & (frm < pieces), lambda d=d, frm=frm: remote(
            span(raw, frm, raw_piece), span(raw, frm, raw_piece), raw_gather + d, {"pcol": frm}))
    for k in range(1, height):
        block = swap(k, raw[pl.ds((k - 1) * side, side)], top[...])
        lower = dot(block, uf[...]).astype(jnp.bfloat16)
        store[slots + k * width] = lower
        for c in panel_cols:
            at = slots + k * width + c
            store[at] = (store[at].astype(jnp.float32) - dot(lower, store[slots + c])).astype(jnp.bfloat16)

    for s in range(slots):
        out_ref[0, 0, s] = store[source[s]]
    for cond, make in ends:
        guard(cond, lambda make=make: make().wait_send())


def body(tiles, tile_ids, counts, pivots, l_inverse, u_inverse):
    rows = lax.axis_size("prow")
    cols = lax.axis_size("pcol")
    side = pivots.shape[0]
    slots = tiles.shape[2]
    grid_cols = LOCAL_ROWS * rows // cols
    levels = rows.bit_length() - 1
    width = UPPER_MOST + 1
    height = LOWER_MOST + 1
    block = (side, side)
    pieces = min(cols, 16)
    count = 3 * rows + 2 * pieces + 3 * cols + width * (2 + 4 * (levels - 1))
    kind = jnp.bfloat16
    hbm = pl.BlockSpec(memory_space=pltpu.HBM)
    return pl.pallas_call(
        functools.partial(kernel, rows, cols, grid_cols),
        out_shape=jax.ShapeDtypeStruct(tiles.shape, tiles.dtype),
        in_specs=[hbm] * 6,
        out_specs=pl.BlockSpec(memory_space=pltpu.VMEM),
        scratch_shapes=[
            pltpu.SMEM(tile_ids.shape, jnp.int32),
            pltpu.SMEM(counts.shape, jnp.int32),
            pltpu.VMEM((1, side), jnp.int32),
            pltpu.VMEM((slots + height * width + 1,) + block, kind),
            pltpu.VMEM((width,) + block, kind),
            pltpu.VMEM((width,) + block, kind),
            pltpu.VMEM((levels - 1, width) + block, kind),
            pltpu.VMEM((levels, width) + block, kind),
            pltpu.VMEM((width,) + block, kind),
            pltpu.VMEM((LOWER_MOST * side, side), kind),
            pltpu.VMEM(block, kind),
            pltpu.VMEM((cols, side // cols, side), kind),
            pltpu.VMEM(block, kind),
            pltpu.VMEM((rows - 1,) + block, kind),
            pltpu.SemaphoreType.DMA((6,)),
            pltpu.SemaphoreType.DMA((count,)),
            pltpu.SemaphoreType.DMA((count,)),
        ],
        compiler_params=pltpu.CompilerParams(
            collective_id=0, has_side_effects=True, vmem_limit_bytes=48 * 1024 * 1024
        ),
    )(tile_ids, counts, pivots.reshape(1, side), l_inverse.T, u_inverse, tiles)


def solution(mesh):
    placed = (
        P("prow", "pcol", None, None, None),
        P("prow", "pcol", None),
        P("prow", "pcol"),
        P(),
        P(None, "pcol"),
        P("prow", None),
    )
    return jax.shard_map(
        body,
        mesh=mesh,
        in_specs=placed,
        out_specs=P("prow", "pcol", None, None, None),
        check_vma=False,
    )
```

```python
import functools

import jax
import jax.numpy as jnp
from jax import lax
from jax.experimental import pallas as pl
from jax.experimental.pallas import tpu as pltpu
from jax.sharding import PartitionSpec as P

LOCAL_ROWS = 16
LOWER_MOST = 3
UPPER_MOST = 3
MESH = pl.DeviceIdType.MESH
NT = (((1,), (1,)), ((), ()))
TN = (((0,), (0,)), ((), ()))
FAR = 1 << 24


def dot(a, b, dims=None):
    if dims is None:
        return jnp.dot(a, b, preferred_element_type=jnp.float32)
    return lax.dot_general(a, b, dims, preferred_element_type=jnp.float32)


def kernel(
    rows, cols, grid_cols,
    counts_ref, ids_hbm, piv_hbm, l_hbm, u_hbm, tiles_hbm,
    out_ref,
    ids_ref, piv_ref,
    store, part, old, send, recv, new, raw, top, lt, uf, corner,
    in_sem, ss, rs,
):
    side = piv_ref.shape[1]
    half = side // 2
    slots = tiles_hbm.shape[2]
    zero_at = store.shape[0] - 1
    levels = rows.bit_length() - 1
    width = UPPER_MOST + 1
    height = LOWER_MOST + 1
    pieces = min(cols, 16)
    panel_cols = range(1, width)
    p = lax.axis_index("prow")
    q = lax.axis_index("pcol")
    core = lax.rem(p, 2)
    used = [0]
    ends = []

    def fresh(n=1):
        used[0] += n
        return used[0] - n

    def remote(src, dst, index, device):
        return pltpu.make_async_remote_copy(
            src_ref=src, dst_ref=dst, send_sem=ss.at[index], recv_sem=rs.at[index],
            device_id=device, device_id_type=MESH,
        )

    def guard(cond, fn):
        if cond is None:
            fn()
        else:
            pl.when(cond)(fn)

    def begin(cond, make):
        guard(cond, lambda: make().start())
        ends.append((cond, make))

    def arrived(cond, make):
        guard(cond, lambda: make().wait_recv())

    def span(buf, at, length):
        return buf.at[pl.ds(pl.multiple_of(at * length, 16), length)]

    u_rows = u_hbm.shape[0]
    tile_copy = pltpu.make_async_copy(tiles_hbm.at[0, 0], store.at[pl.ds(0, slots)], in_sem.at[0])
    inputs = [
        pltpu.make_async_copy(ids_hbm, ids_ref, in_sem.at[1]),
        pltpu.make_async_copy(piv_hbm, piv_ref, in_sem.at[3]),
        pltpu.make_async_copy(l_hbm, lt.at[q], in_sem.at[4]),
        pltpu.make_async_copy(u_hbm, span(uf, p, u_rows), in_sem.at[5]),
    ]
    for copy in inputs[:2]:
        copy.start()
    tile_copy.start()
    for copy in inputs[2:]:
        copy.start()

    barrier = pltpu.get_barrier_semaphore()
    for d in range(1, rows):
        pl.semaphore_signal(barrier, inc=1, device_id={"prow": lax.rem(p + d, rows)}, device_id_type=MESH)
    for d in range(1, cols):
        pl.semaphore_signal(barrier, inc=1, device_id={"pcol": lax.rem(q + d, cols)}, device_id_type=MESH)
    store[zero_at] = jnp.zeros((side, side), jnp.bfloat16)
    for copy in inputs:
        copy.wait()

    first_row = LOCAL_ROWS - LOWER_MOST
    first_col = grid_cols - UPPER_MOST
    packed = [jnp.int32(0)] * height
    source = []
    live_count = counts_ref[0, 0]
    for s in range(slots):
        code = ids_ref[0, 0, s]
        row = code // grid_cols
        col = code - row * grid_cols
        live = s < live_count
        c = jnp.where((col == 0) & (q == 0), 0, jnp.where(col >= first_col, col - first_col + 1, -1))
        k = jnp.where((row == 0) & (p == 0), 0, jnp.where(row >= first_row, row - first_row + 1, -1))
        weight = jnp.int32(0)
        for j in range(width):
            weight = jnp.where(c == j, (s + 1) << (5 * j), weight)
        for i in range(height):
            packed[i] = packed[i] + jnp.where((k == i) & live, weight, 0)
        structural = (c >= 0) & (k >= 0)
        source.append(jnp.where(live, jnp.where(structural, slots + k * width + c, s), zero_at))

    def tile(k, c):
        slot = (packed[k] >> (5 * c)) & 31
        return store[jnp.where(slot > 0, slot - 1, zero_at)]

    piv_lanes = jnp.broadcast_to(piv_ref[...], (side, side))
    piv_rows = piv_lanes.T
    lane = lax.broadcasted_iota(jnp.int32, (side, side), 1)
    sub = lax.broadcasted_iota(jnp.int32, (side, side), 0)
    base = [jnp.where(p == 0, 0, -FAR)]
    for i in range(LOWER_MOST):
        base.append((p + rows * (first_row + i)) * side)
    pick = [(piv_rows == lane + b).astype(jnp.float32).astype(jnp.bfloat16) for b in base]
    owner_high = lax.rem(piv_rows // side, rows) >= rows // 2
    mine_high = p >= rows // 2
    same = owner_high.astype(jnp.int32) == mine_high.astype(jnp.int32)

    tile_copy.wait()

    @pl.when(q == 0)
    def _():
        for i in range(LOWER_MOST):
            raw[pl.ds(i * side, side)] = tile(i + 1, 0)

        @pl.when(p == 0)
        def _():
            top[...] = tile(0, 0)

    pl.semaphore_wait(barrier, rows + cols - 2)

    top_piece = side // pieces
    raw_piece = LOWER_MOST * side // pieces
    top_scatter, raw_scatter = fresh(pieces), fresh(pieces)
    top_spread = fresh(rows)
    top_gather, raw_gather = fresh(cols), fresh(cols)
    for j in range(pieces - 1, 0, -1):
        begin((q == 0) & (p == 0), lambda j=j: remote(
            span(top, j, top_piece), span(top, j, top_piece), top_scatter + j, {"pcol": j}))
    for j in range(pieces - 1, 0, -1):
        begin(q == 0, lambda j=j: remote(
            span(raw, j, raw_piece), span(raw, j, raw_piece), raw_scatter + j, {"pcol": j}))

    partner = {"prow": p + 1 - 2 * core}
    level0 = [fresh(2) for c in range(width)]

    def contribute(c):
        total = dot(pick[0], tile(0, c))
        for k in range(1, height):
            total = total + dot(pick[k], tile(k, c))
        part[c] = total.astype(jnp.bfloat16)

    for c in panel_cols:
        contribute(c)

        @pl.when(p == 0)
        def _():
            old[c] = tile(0, c)

        begin(None, lambda c=c: remote(part.at[c], recv.at[0, c], level0[c], partner))
        begin(p == 0, lambda c=c: remote(old.at[c], old.at[c], level0[c] + 1, {"prow": 1}))

    def low(level):
        return p < (1 << level)

    def high(level):
        return (p >= (1 << level)) & (p < (2 << level))

    sems = {}

    def level_send(level, c):
        peer = {"prow": p + (1 << level) - 2 * (1 << level) * lax.rem(p // (1 << level), 2)}
        last = level == levels - 1
        sems[level, c] = fresh(4)
        index = sems[level, c]
        before = part if level == 1 else send.at[level - 2]
        if level == 1:
            arrived(p == 1, lambda: remote(old.at[c], old.at[c], level0[c] + 1, {"prow": 0}))
            arrived(None, lambda: remote(part.at[c], recv.at[0, c], level0[c], partner))
        total = before[c].astype(jnp.float32) + recv[level - 1, c].astype(jnp.float32)
        send[level - 1, c] = total.astype(jnp.bfloat16)
        if last:
            @pl.when(p < rows // 2)
            def _():
                new[c] = jnp.where(owner_high, old[c].astype(jnp.float32), total).astype(jnp.bfloat16)

            @pl.when(p >= rows // 2)
            def _():
                new[c] = total.astype(jnp.bfloat16)

        src = new.at[c] if last else send.at[level - 1, c]
        begin(None, lambda: remote(span(src, core, half), span(recv.at[level, c], core, half), index, peer))
        if not last:
            begin(low(level),
                  lambda: remote(span(old.at[c], core, half), span(old.at[c], core, half), index + 1, peer))

    def level_forward(level, c):
        index = sems[level, c]
        here = span(recv.at[level, c], core, half)
        arrived(None, lambda: remote(here, here, index, partner))
        begin(None, lambda: remote(here, here, index + 2, partner))
        if level < levels - 1:
            mine = span(old.at[c], core, half)
            arrived(high(level), lambda: remote(mine, mine, index + 1, partner))
            begin(high(level), lambda: remote(mine, mine, index + 3, partner))

    def level_done(level, c):
        index = sems[level, c]
        there = span(recv.at[level, c], 1 - core, half)
        arrived(None, lambda: remote(there, there, index + 2, partner))
        if level < levels - 1:
            theirs = span(old.at[c], 1 - core, half)
            arrived(high(level), lambda: remote(theirs, theirs, index + 3, partner))

    for c in panel_cols:
        level_send(1, c)

    for j in range(1, pieces):
        arrived((q == j) & (p == 0), lambda j=j: remote(
            span(top, j, top_piece), span(top, j, top_piece), top_scatter + j, {"pcol": 0}))
    mine_top = span(top, q, top_piece)
    for d in range(1, rows):
        begin((p == 0) & (q < pieces), lambda d=d: remote(mine_top, mine_top, top_spread + d, {"prow": d}))

    def top_relay(cond):
        for d in range(1, cols):
            to = lax.rem(q + d, cols)
            begin(cond & (q < pieces) & ((to != 0) | (p != 0)),
                  lambda d=d, to=to: remote(mine_top, mine_top, top_gather + d, {"pcol": to}))

    for j in range(1, pieces):
        arrived(q == j, lambda j=j: remote(
            span(raw, j, raw_piece), span(raw, j, raw_piece), raw_scatter + j, {"pcol": 0}))
    mine_raw = span(raw, q, raw_piece)
    for d in range(1, cols):
        to = lax.rem(q + d, cols)
        begin((q < pieces) & (to != 0),
              lambda d=d, to=to: remote(mine_raw, mine_raw, raw_gather + d, {"pcol": to}))
    for d in range(1, rows):
        arrived((p == d) & (q < pieces), lambda d=d: remote(mine_top, mine_top, top_spread + d, {"prow": 0}))
    top_relay(p >= 0)

    l_sem, u_sem, corner_sem = fresh(cols), fresh(rows), fresh(rows)
    for d in range(1, cols):
        begin(None, lambda d=d: remote(lt.at[q], lt.at[q], l_sem + d, {"pcol": lax.rem(q + d, cols)}))
    mine_u = span(uf, p, u_rows)
    for d in range(1, rows):
        begin(None, lambda d=d: remote(mine_u, mine_u, u_sem + d, {"prow": lax.rem(p + d, rows)}))

    @pl.when(q == 0)
    def _():
        contribute(0)

    for d in range(1, rows):
        begin((q == 0) & (p == d), lambda d=d: remote(part.at[0], corner.at[d - 1], corner_sem + d, {"prow": 0}))

    for level in range(1, levels):
        if level > 1:
            for c in panel_cols:
                level_send(level, c)
        for c in panel_cols:
            level_forward(level, c)
        if level < levels - 1:
            for c in panel_cols:
                level_done(level, c)

    for d in range(1, cols):
        frm = lax.rem(q + cols - d, cols)
        remote(lt.at[frm], lt.at[frm], l_sem + d, {"pcol": frm}).wait_recv()
    lower_t = lt[...].astype(jnp.float32).reshape(side, side).astype(jnp.bfloat16)

    hit = [piv_lanes == sub + b for b in base]
    moved = [jnp.max(h.astype(jnp.float32), axis=1, keepdims=True) > 0.5 for h in hit]
    choose = [h.astype(jnp.float32).astype(jnp.bfloat16) for h in hit]

    def swap(k, block, source_rows):
        return jnp.where(moved[k], dot(choose[k], source_rows), block.astype(jnp.float32)).astype(jnp.bfloat16)

    for c in panel_cols:
        level_done(levels - 1, c)
        fresh_top = jnp.where(same, send[levels - 2, c].astype(jnp.float32),
                              recv[levels - 1, c].astype(jnp.float32)).astype(jnp.bfloat16)
        store[slots + c] = dot(lower_t, fresh_top, TN).astype(jnp.bfloat16)

        @pl.when(mine_high)
        def _():
            old[c] = recv[levels - 1, c]

        for k in range(1, height):
            store[slots + k * width + c] = swap(k, tile(k, c), old[c])

    for d in range(1, rows):
        frm = lax.rem(p + rows - d, rows)
        there = span(uf, frm, u_rows)
        remote(there, there, u_sem + d, {"prow": frm}).wait_recv()

    @pl.when((q == 0) & (p == 0))
    def _():
        total = part[0].astype(jnp.float32)
        for d in range(1, rows):
            remote(part.at[0], corner.at[d - 1], corner_sem + d, {"prow": d}).wait_recv()
            total = total + corner[d - 1].astype(jnp.float32)
        store[slots] = total.astype(jnp.bfloat16)

    for d in range(1, cols):
        frm = lax.rem(q + cols - d, cols)
        arrived((frm < pieces) & ((q != 0) | (p != 0)), lambda d=d, frm=frm: remote(
            span(top, frm, top_piece), span(top, frm, top_piece), top_gather + d, {"pcol": frm}))
    for d in range(1, cols):
        frm = lax.rem(q + cols - d, cols)
        arrived((q != 0) & (frm < pieces), lambda d=d, frm=frm: remote(
            span(raw, frm, raw_piece), span(raw, frm, raw_piece), raw_gather + d, {"pcol": frm}))
    for k in range(1, height):
        block = swap(k, raw[pl.ds((k - 1) * side, side)], top[...])
        lower = dot(block, uf[...]).astype(jnp.bfloat16)
        store[slots + k * width] = lower
        for c in panel_cols:
            at = slots + k * width + c
            store[at] = (store[at].astype(jnp.float32) - dot(lower, store[slots + c])).astype(jnp.bfloat16)

    for s in range(slots):
        out_ref[0, 0, s] = store[source[s]]
    for cond, make in ends:
        guard(cond, lambda make=make: make().wait_send())


def body(tiles, tile_ids, counts, pivots, l_inverse, u_inverse):
    rows = lax.axis_size("prow")
    cols = lax.axis_size("pcol")
    side = pivots.shape[0]
    slots = tiles.shape[2]
    grid_cols = LOCAL_ROWS * rows // cols
    levels = rows.bit_length() - 1
    width = UPPER_MOST + 1
    height = LOWER_MOST + 1
    block = (side, side)
    pieces = min(cols, 16)
    count = 3 * rows + 2 * pieces + 3 * cols + width * (2 + 4 * (levels - 1))
    kind = jnp.bfloat16
    operands = (tile_ids, pivots.reshape(1, side), l_inverse.T, u_inverse, tiles)
    hbm = pl.BlockSpec(memory_space=pltpu.HBM)
    return pl.pallas_call(
        functools.partial(kernel, rows, cols, grid_cols),
        out_shape=jax.ShapeDtypeStruct(tiles.shape, tiles.dtype),
        in_specs=[pl.BlockSpec(memory_space=pltpu.SMEM)] + [hbm] * 5,
        out_specs=pl.BlockSpec(memory_space=pltpu.VMEM),
        scratch_shapes=[
            pltpu.SMEM(tile_ids.shape, jnp.int32),
            pltpu.VMEM((1, side), jnp.int32),
            pltpu.VMEM((slots + height * width + 1,) + block, kind),
            pltpu.VMEM((width,) + block, kind),
            pltpu.VMEM((width,) + block, kind),
            pltpu.VMEM((levels - 1, width) + block, kind),
            pltpu.VMEM((levels, width) + block, kind),
            pltpu.VMEM((width,) + block, kind),
            pltpu.VMEM((LOWER_MOST * side, side), kind),
            pltpu.VMEM(block, kind),
            pltpu.VMEM((cols, side // cols, side), kind),
            pltpu.VMEM(block, kind),
            pltpu.VMEM((rows - 1,) + block, kind),
            pltpu.SemaphoreType.DMA((6,)),
            pltpu.SemaphoreType.DMA((count,)),
            pltpu.SemaphoreType.DMA((count,)),
        ],
        compiler_params=pltpu.CompilerParams(
            collective_id=0, has_side_effects=True, vmem_limit_bytes=48 * 1024 * 1024
        ),
    )(counts, *[pltpu.with_memory_space_constraint(a, pltpu.HBM) for a in operands])


def solution(mesh):
    placed = (
        P("prow", "pcol", None, None, None),
        P("prow", "pcol", None),
        P("prow", "pcol"),
        P(),
        P(None, "pcol"),
        P("prow", None),
    )
    return jax.shard_map(
        body,
        mesh=mesh,
        in_specs=placed,
        out_specs=P("prow", "pcol", None, None, None),
        check_vma=False,
    )
```

```python
import functools

import jax
import jax.numpy as jnp
from jax import lax
from jax.experimental import pallas as pl
from jax.experimental.pallas import tpu as pltpu
from jax.sharding import PartitionSpec as P

LOCAL_ROWS = 16
LOWER_MOST = 3
UPPER_MOST = 3
MESH = pl.DeviceIdType.MESH
NT = (((1,), (1,)), ((), ()))
TN = (((0,), (0,)), ((), ()))
FAR = 1 << 24


def dot(a, b, dims=None):
    if dims is None:
        return jnp.dot(a, b, preferred_element_type=jnp.float32)
    return lax.dot_general(a, b, dims, preferred_element_type=jnp.float32)


def kernel(
    rows, cols, grid_cols,
    counts_ref, ids_hbm, piv_hbm, l_hbm, u_hbm, tiles_hbm,
    out_ref,
    ids_ref, piv_ref,
    store, part, old, send, recv, new, raw, top, lt, uf, corner,
    in_sem, ss, rs,
):
    side = piv_ref.shape[1]
    half = side // 2
    slots = tiles_hbm.shape[2]
    zero_at = store.shape[0] - 1
    levels = rows.bit_length() - 1
    width = UPPER_MOST + 1
    height = LOWER_MOST + 1
    pieces = min(cols, 16)
    panel_cols = range(1, width)
    p = lax.axis_index("prow")
    q = lax.axis_index("pcol")
    core = lax.rem(p, 2)
    used = [0]
    ends = []

    def fresh(n=1):
        used[0] += n
        return used[0] - n

    def remote(src, dst, index, device):
        return pltpu.make_async_remote_copy(
            src_ref=src, dst_ref=dst, send_sem=ss.at[index], recv_sem=rs.at[index],
            device_id=device, device_id_type=MESH,
        )

    def guard(cond, fn):
        if cond is None:
            fn()
        else:
            pl.when(cond)(fn)

    def begin(cond, make):
        guard(cond, lambda: make().start())
        ends.append((cond, make))

    def arrived(cond, make):
        guard(cond, lambda: make().wait_recv())

    def span(buf, at, length):
        return buf.at[pl.ds(pl.multiple_of(at * length, 16), length)]

    u_rows = u_hbm.shape[0]
    tile_copy = pltpu.make_async_copy(tiles_hbm.at[0, 0], store.at[pl.ds(0, slots)], in_sem.at[0])
    inputs = [
        pltpu.make_async_copy(ids_hbm, ids_ref, in_sem.at[1]),
        pltpu.make_async_copy(piv_hbm, piv_ref, in_sem.at[3]),
        pltpu.make_async_copy(l_hbm, lt.at[q], in_sem.at[4]),
        pltpu.make_async_copy(u_hbm, span(uf, p, u_rows), in_sem.at[5]),
    ]
    for copy in inputs[:2]:
        copy.start()
    tile_copy.start()
    for copy in inputs[2:]:
        copy.start()

    barrier = pltpu.get_barrier_semaphore()
    for d in range(1, rows):
        pl.semaphore_signal(barrier, inc=1, device_id={"prow": lax.rem(p + d, rows)}, device_id_type=MESH)
    for d in range(1, cols):
        pl.semaphore_signal(barrier, inc=1, device_id={"pcol": lax.rem(q + d, cols)}, device_id_type=MESH)
    store[zero_at] = jnp.zeros((side, side), jnp.bfloat16)
    for copy in inputs:
        copy.wait()

    first_row = LOCAL_ROWS - LOWER_MOST
    first_col = grid_cols - UPPER_MOST
    packed = [jnp.int32(0)] * height
    source = []
    live_count = counts_ref[0, 0]
    for s in range(slots):
        code = ids_ref[0, 0, s]
        row = code // grid_cols
        col = code - row * grid_cols
        live = s < live_count
        c = jnp.where((col == 0) & (q == 0), 0, jnp.where(col >= first_col, col - first_col + 1, -1))
        k = jnp.where((row == 0) & (p == 0), 0, jnp.where(row >= first_row, row - first_row + 1, -1))
        weight = jnp.int32(0)
        for j in range(width):
            weight = jnp.where(c == j, (s + 1) << (5 * j), weight)
        for i in range(height):
            packed[i] = packed[i] + jnp.where((k == i) & live, weight, 0)
        structural = (c >= 0) & (k >= 0)
        source.append(jnp.where(live, jnp.where(structural, slots + k * width + c, s), zero_at))

    def tile(k, c):
        slot = (packed[k] >> (5 * c)) & 31
        return store[jnp.where(slot > 0, slot - 1, zero_at)]

    piv_lanes = jnp.broadcast_to(piv_ref[...], (side, side))
    piv_rows = piv_lanes.T
    lane = lax.broadcasted_iota(jnp.int32, (side, side), 1)
    sub = lax.broadcasted_iota(jnp.int32, (side, side), 0)
    base = [jnp.where(p == 0, 0, -FAR)]
    for i in range(LOWER_MOST):
        base.append((p + rows * (first_row + i)) * side)
    pick = [(piv_rows == lane + b).astype(jnp.float32).astype(jnp.bfloat16) for b in base]
    owner_high = lax.rem(piv_rows // side, rows) >= rows // 2
    mine_high = p >= rows // 2
    same = owner_high.astype(jnp.int32) == mine_high.astype(jnp.int32)

    tile_copy.wait()

    @pl.when(q == 0)
    def _():
        for i in range(LOWER_MOST):
            raw[pl.ds(i * side, side)] = tile(i + 1, 0)

        @pl.when(p == 0)
        def _():
            top[...] = tile(0, 0)

    pl.semaphore_wait(barrier, rows + cols - 2)

    top_piece = side // pieces
    raw_piece = LOWER_MOST * side // pieces
    top_scatter, raw_scatter = fresh(pieces), fresh(pieces)
    top_spread = fresh(rows)
    top_gather, raw_gather = fresh(cols), fresh(cols)
    for j in range(pieces - 1, 0, -1):
        begin((q == 0) & (p == 0), lambda j=j: remote(
            span(top, j, top_piece), span(top, j, top_piece), top_scatter + j, {"pcol": j}))
    for j in range(pieces - 1, 0, -1):
        begin(q == 0, lambda j=j: remote(
            span(raw, j, raw_piece), span(raw, j, raw_piece), raw_scatter + j, {"pcol": j}))

    partner = {"prow": p + 1 - 2 * core}
    level0 = [fresh(2) for c in range(width)]

    def contribute(c):
        total = dot(pick[0], tile(0, c))
        for k in range(1, height):
            total = total + dot(pick[k], tile(k, c))
        part[c] = total.astype(jnp.bfloat16)

    for c in panel_cols:
        contribute(c)

        @pl.when(p == 0)
        def _():
            old[c] = tile(0, c)

        begin(None, lambda c=c: remote(part.at[c], recv.at[0, c], level0[c], partner))
        begin(p == 0, lambda c=c: remote(old.at[c], old.at[c], level0[c] + 1, {"prow": 1}))

    def low(level):
        return p < (1 << level)

    def high(level):
        return (p >= (1 << level)) & (p < (2 << level))

    sems = {}

    def level_send(level, c):
        peer = {"prow": p + (1 << level) - 2 * (1 << level) * lax.rem(p // (1 << level), 2)}
        last = level == levels - 1
        sems[level, c] = fresh(4)
        index = sems[level, c]
        before = part if level == 1 else send.at[level - 2]
        if level == 1:
            arrived(p == 1, lambda: remote(old.at[c], old.at[c], level0[c] + 1, {"prow": 0}))
            arrived(None, lambda: remote(part.at[c], recv.at[0, c], level0[c], partner))
        total = before[c].astype(jnp.float32) + recv[level - 1, c].astype(jnp.float32)
        send[level - 1, c] = total.astype(jnp.bfloat16)
        if last:
            @pl.when(p < rows // 2)
            def _():
                new[c] = jnp.where(owner_high, old[c].astype(jnp.float32), total).astype(jnp.bfloat16)

            @pl.when(p >= rows // 2)
            def _():
                new[c] = total.astype(jnp.bfloat16)

        src = new.at[c] if last else send.at[level - 1, c]
        begin(None, lambda: remote(span(src, core, half), span(recv.at[level, c], core, half), index, peer))
        if not last:
            begin(low(level),
                  lambda: remote(span(old.at[c], core, half), span(old.at[c], core, half), index + 1, peer))

    def level_forward(level, c):
        index = sems[level, c]
        here = span(recv.at[level, c], core, half)
        arrived(None, lambda: remote(here, here, index, partner))
        begin(None, lambda: remote(here, here, index + 2, partner))
        if level < levels - 1:
            mine = span(old.at[c], core, half)
            arrived(high(level), lambda: remote(mine, mine, index + 1, partner))
            begin(high(level), lambda: remote(mine, mine, index + 3, partner))

    def level_done(level, c):
        index = sems[level, c]
        there = span(recv.at[level, c], 1 - core, half)
        arrived(None, lambda: remote(there, there, index + 2, partner))
        if level < levels - 1:
            theirs = span(old.at[c], 1 - core, half)
            arrived(high(level), lambda: remote(theirs, theirs, index + 3, partner))

    for c in panel_cols:
        level_send(1, c)

    for j in range(1, pieces):
        arrived((q == j) & (p == 0), lambda j=j: remote(
            span(top, j, top_piece), span(top, j, top_piece), top_scatter + j, {"pcol": 0}))
    mine_top = span(top, q, top_piece)
    for d in range(1, rows):
        begin((p == 0) & (q < pieces), lambda d=d: remote(mine_top, mine_top, top_spread + d, {"prow": d}))

    def top_relay(cond):
        for d in range(1, cols):
            to = lax.rem(q + d, cols)
            begin(cond & (q < pieces) & ((to != 0) | (p != 0)),
                  lambda d=d, to=to: remote(mine_top, mine_top, top_gather + d, {"pcol": to}))

    for j in range(1, pieces):
        arrived(q == j, lambda j=j: remote(
            span(raw, j, raw_piece), span(raw, j, raw_piece), raw_scatter + j, {"pcol": 0}))
    mine_raw = span(raw, q, raw_piece)
    twin = q + 1 - 2 * lax.rem(q, 2)
    raw_twin = fresh(cols)
    begin((q < pieces) & (twin != 0), lambda: remote(mine_raw, mine_raw, raw_twin, {"pcol": twin}))
    for d in range(2, cols, 2):
        to = lax.rem(q + d, cols)
        begin((q < pieces) & (to != 0),
              lambda d=d, to=to: remote(mine_raw, mine_raw, raw_gather + d, {"pcol": to}))
    for d in range(1, rows):
        arrived((p == d) & (q < pieces), lambda d=d: remote(mine_top, mine_top, top_spread + d, {"prow": 0}))
    top_relay(p >= 0)

    l_sem, u_sem, corner_sem = fresh(cols), fresh(rows), fresh(rows)
    for d in range(1, cols):
        begin(None, lambda d=d: remote(lt.at[q], lt.at[q], l_sem + d, {"pcol": lax.rem(q + d, cols)}))
    mine_u = span(uf, p, u_rows)
    for d in range(1, rows):
        begin(None, lambda d=d: remote(mine_u, mine_u, u_sem + d, {"prow": lax.rem(p + d, rows)}))

    @pl.when(q == 0)
    def _():
        contribute(0)

    for d in range(1, rows):
        begin((q == 0) & (p == d), lambda d=d: remote(part.at[0], corner.at[d - 1], corner_sem + d, {"prow": 0}))

    for level in range(1, levels):
        if level > 1:
            for c in panel_cols:
                level_send(level, c)
        for c in panel_cols:
            level_forward(level, c)
        if level < levels - 1:
            for c in panel_cols:
                level_done(level, c)

    for d in range(2, cols, 2):
        frm = lax.rem(q + cols - d, cols)
        there = span(raw, frm, raw_piece)
        arrived((q != 0) & (frm < pieces), lambda d=d, there=there, frm=frm: remote(
            there, there, raw_gather + d, {"pcol": frm}))
        begin((twin != 0) & (frm < pieces), lambda d=d, there=there: remote(
            there, there, raw_twin + d, {"pcol": twin}))

    for d in range(1, cols):
        frm = lax.rem(q + cols - d, cols)
        remote(lt.at[frm], lt.at[frm], l_sem + d, {"pcol": frm}).wait_recv()
    lower_t = lt[...].astype(jnp.float32).reshape(side, side).astype(jnp.bfloat16)

    hit = [piv_lanes == sub + b for b in base]
    moved = [jnp.max(h.astype(jnp.float32), axis=1, keepdims=True) > 0.5 for h in hit]
    choose = [h.astype(jnp.float32).astype(jnp.bfloat16) for h in hit]

    def swap(k, block, source_rows):
        return jnp.where(moved[k], dot(choose[k], source_rows), block.astype(jnp.float32)).astype(jnp.bfloat16)

    for c in panel_cols:
        level_done(levels - 1, c)
        fresh_top = jnp.where(same, send[levels - 2, c].astype(jnp.float32),
                              recv[levels - 1, c].astype(jnp.float32)).astype(jnp.bfloat16)
        store[slots + c] = dot(lower_t, fresh_top, TN).astype(jnp.bfloat16)

        @pl.when(mine_high)
        def _():
            old[c] = recv[levels - 1, c]

        for k in range(1, height):
            store[slots + k * width + c] = swap(k, tile(k, c), old[c])

    for d in range(1, rows):
        frm = lax.rem(p + rows - d, rows)
        there = span(uf, frm, u_rows)
        remote(there, there, u_sem + d, {"prow": frm}).wait_recv()

    @pl.when((q == 0) & (p == 0))
    def _():
        total = part[0].astype(jnp.float32)
        for d in range(1, rows):
            remote(part.at[0], corner.at[d - 1], corner_sem + d, {"prow": d}).wait_recv()
            total = total + corner[d - 1].astype(jnp.float32)
        store[slots] = total.astype(jnp.bfloat16)

    for d in range(1, cols):
        frm = lax.rem(q + cols - d, cols)
        arrived((frm < pieces) & ((q != 0) | (p != 0)), lambda d=d, frm=frm: remote(
            span(top, frm, top_piece), span(top, frm, top_piece), top_gather + d, {"pcol": frm}))
    for d in range(0, cols, 2):
        frm = lax.rem(twin + cols - d, cols)
        there = span(raw, frm, raw_piece)
        arrived((q != 0) & (frm < pieces), lambda d=d, there=there: remote(
            there, there, raw_twin + d, {"pcol": twin}))
    for k in range(1, height):
        block = swap(k, raw[pl.ds((k - 1) * side, side)], top[...])
        lower = dot(block, uf[...]).astype(jnp.bfloat16)
        store[slots + k * width] = lower
        for c in panel_cols:
            at = slots + k * width + c
            store[at] = (store[at].astype(jnp.float32) - dot(lower, store[slots + c])).astype(jnp.bfloat16)

    for s in range(slots):
        out_ref[0, 0, s] = store[source[s]]
    for cond, make in ends:
        guard(cond, lambda make=make: make().wait_send())


def body(tiles, tile_ids, counts, pivots, l_inverse, u_inverse):
    rows = lax.axis_size("prow")
    cols = lax.axis_size("pcol")
    side = pivots.shape[0]
    slots = tiles.shape[2]
    grid_cols = LOCAL_ROWS * rows // cols
    levels = rows.bit_length() - 1
    width = UPPER_MOST + 1
    height = LOWER_MOST + 1
    block = (side, side)
    pieces = min(cols, 16)
    count = 3 * rows + 2 * pieces + 4 * cols + width * (2 + 4 * (levels - 1))
    kind = jnp.bfloat16
    operands = (tile_ids, pivots.reshape(1, side), l_inverse.T, u_inverse, tiles)
    hbm = pl.BlockSpec(memory_space=pltpu.HBM)
    return pl.pallas_call(
        functools.partial(kernel, rows, cols, grid_cols),
        out_shape=jax.ShapeDtypeStruct(tiles.shape, tiles.dtype),
        in_specs=[pl.BlockSpec(memory_space=pltpu.SMEM)] + [hbm] * 5,
        out_specs=pl.BlockSpec(memory_space=pltpu.VMEM),
        scratch_shapes=[
            pltpu.SMEM(tile_ids.shape, jnp.int32),
            pltpu.VMEM((1, side), jnp.int32),
            pltpu.VMEM((slots + height * width + 1,) + block, kind),
            pltpu.VMEM((width,) + block, kind),
            pltpu.VMEM((width,) + block, kind),
            pltpu.VMEM((levels - 1, width) + block, kind),
            pltpu.VMEM((levels, width) + block, kind),
            pltpu.VMEM((width,) + block, kind),
            pltpu.VMEM((LOWER_MOST * side, side), kind),
            pltpu.VMEM(block, kind),
            pltpu.VMEM((cols, side // cols, side), kind),
            pltpu.VMEM(block, kind),
            pltpu.VMEM((rows - 1,) + block, kind),
            pltpu.SemaphoreType.DMA((6,)),
            pltpu.SemaphoreType.DMA((count,)),
            pltpu.SemaphoreType.DMA((count,)),
        ],
        compiler_params=pltpu.CompilerParams(
            collective_id=0, has_side_effects=True, vmem_limit_bytes=48 * 1024 * 1024
        ),
    )(counts, *[pltpu.with_memory_space_constraint(a, pltpu.HBM) for a in operands])


def solution(mesh):
    placed = (
        P("prow", "pcol", None, None, None),
        P("prow", "pcol", None),
        P("prow", "pcol"),
        P(),
        P(None, "pcol"),
        P("prow", None),
    )
    return jax.shard_map(
        body,
        mesh=mesh,
        in_specs=placed,
        out_specs=P("prow", "pcol", None, None, None),
        check_vma=False,
    )
```
